128 devices in a mesh: groups: 4 (over x, y), seq: 32 (over z, core).
Axes of the slice: x: 2, y: 2, z: 16, core: 2. Of those that a mesh axis runs over, the one named last changes fastest.
The devices are a block of a 8x8x16 slice.
Arguments:
- queries: bfloat16 [8192, 24576], P(('groups', 'seq')), parts along dimension 0, may hold values from -500 to 500
- kv_new: bfloat16 [8192, 576], P(('groups', 'seq')), parts along dimension 0, may hold values from -6 to 6
- kv_cache: bfloat16 [4096, 576], P(('groups', 'seq')), parts along dimension 0, may hold values from -6 to 6
- kv_gain: float32 [512], replicated, may hold values from 0.5 to 2
- w_key: bfloat16 [512, 16384], P(None, 'seq'), may hold values from -0.25 to 0.25
- w_value: bfloat16 [512, 16384], P(None, 'seq'), may hold values from -0.25 to 0.25
- prefix_len: int32 [4], P('groups'), parts along dimension 0, may hold values from 256 to 1024
Outputs:
- attended: bfloat16 [8192, 16384], P(('groups', 'seq')), parts along dimension 0
The draws below stay inside these ranges and needn't reach their ends.
There are 4 independent parts, one for each index of `groups`. The reference program is written for one: setup_inputs(seed, part) draws one part's arguments, and reference() takes and returns one part's arrays. A program takes and returns all parts, laid end to end along the dimension named above; an argument that names none is the same for every part. Nothing has to cross between parts.
Inputs may be any that keep to these rules, and one draw needn't show every extreme that they name: The stretch's tokens take positions from prefix_len on.
All inputs are finite; a program needn't handle non-finite values.
Results may differ from the reference program's by a relative error of at most 0.012.
Values may be sent and summed in bfloat16 or wider, within the bound.
A program may use at most 128 MiB of HBM per device.

```python
import math
import jax
import jax.numpy as jnp
from jax import lax

H = 128
NOPE = 128
ROPE = 64
LATENT = 512
VH = 128
TOKENS = 2048
CACHE = 1024


def draw_queries(key, part):
    base_key = jax.random.fold_in(jax.random.fold_in(key, 11), 0)
    values = jnp.clip(jax.random.normal(base_key, (TOKENS, H * (NOPE + ROPE)), jnp.float32), -8.0, 8.0)
    return values.astype(jnp.bfloat16)


def block_scale(rng, extent, shards, least, top_value):
    def one(position, blocks):
        draws = jax.random.uniform(jax.random.fold_in(jax.random.fold_in(rng, 6), position), (blocks,), jnp.float32, least / len(shards), top_value / len(shards))
        return jnp.repeat(jnp.exp(draws), extent[position] // blocks).reshape((-1,) + (1,) * (len(extent) - position - 1))

    loudness = one(*shards[0])
    for cut in shards[1:]:
        loudness = loudness * one(*cut)
    return loudness


def normal_values(stream_key, extent, deviation, reach, cuts=(), kind=jnp.bfloat16):
    result = deviation * jax.random.normal(stream_key, extent, jnp.float32)
    if cuts:
        result = result * block_scale(stream_key, extent, cuts, -0.22, 0.18)
    return jnp.clip(result, -reach, reach).astype(kind)


def setup_inputs(seed: int = 0, part: int = 0) -> dict:
    arg_keys = jax.random.split(jax.random.key(seed), 8)
    part_splits = jax.random.split(jax.random.fold_in(arg_keys[7], part), 8)
    return {
        "queries": draw_queries(jax.random.fold_in(jax.random.fold_in(arg_keys[7], part), 71), part),
        "kv_new": normal_values(part_splits[1], (TOKENS, LATENT + ROPE), 1.0, 6.0, ((0, 32),)),
        "kv_cache": normal_values(part_splits[2], (CACHE, LATENT + ROPE), 1.0, 6.0, ((0, 32),)),
        "kv_gain": jnp.clip(jnp.exp(jax.random.uniform(arg_keys[3], (LATENT,), jnp.float32, math.log(0.5), math.log(2.0))), 0.5, 2.0),
        "w_key": normal_values(arg_keys[4], (LATENT, H * NOPE), LATENT ** -0.5, 0.25, ((1, 32),)),
        "w_value": normal_values(arg_keys[5], (LATENT, H * VH), LATENT ** -0.5, 0.25, ((1, 32),)),
        "prefix_len": jax.random.randint(part_splits[6], (1,), CACHE // 4, CACHE + 1).astype(jnp.int32),
    }


epsilon = 1e-06

def phases_for(positions, rope_width):
    half_width = rope_width // 2
    inverse = 10000.0 ** (-(jnp.arange(half_width, dtype=jnp.float32) * 2.0) / rope_width)
    return positions.astype(jnp.float32)[:, None] * inverse[None, :]

def rotate(values, phases):
    half_width = values.shape[-1] // 2
    front_half = values[..., :half_width]
    back_half = values[..., half_width:]
    cosine = jnp.cos(phases)
    sine_part = jnp.sin(phases)
    return jnp.concatenate([front_half * cosine - back_half * sine_part, back_half * cosine + front_half * sine_part], -1)

def reference(queries, kv_new, kv_cache, kv_gain, w_key, w_value, prefix_len):
    stretch_start = prefix_len[0]
    tokens_all = queries.shape[0]
    cached_all = kv_cache.shape[0]
    positions = stretch_start + jnp.arange(tokens_all, dtype=jnp.int32)
    phases = phases_for(positions, ROPE)
    raw_latent = kv_new[:, :LATENT].astype(jnp.float32)
    inv_rms = lax.rsqrt(lax.optimization_barrier(jnp.mean(raw_latent * raw_latent, axis=1, keepdims=True)) + epsilon)
    latent_new = (raw_latent * inv_rms * kv_gain[None, :]).astype(jnp.bfloat16)
    rope_new = rotate(kv_new[:, LATENT:].astype(jnp.float32), phases).astype(jnp.bfloat16)
    keys_all = jnp.concatenate([kv_cache, jnp.concatenate([latent_new, rope_new], 1)], 0)
    latent_all = keys_all[:, :LATENT]
    key_rope = keys_all[:, LATENT:]
    query_heads = queries.reshape(tokens_all, H, NOPE + ROPE)
    query_rot = rotate(query_heads[:, :, NOPE:].astype(jnp.float32), phases[:, None, :]).astype(jnp.bfloat16)
    query_nope = jnp.transpose(query_heads[:, :, :NOPE], (1, 0, 2))
    query_rot = jnp.transpose(query_rot, (1, 0, 2))
    key_maps = jnp.transpose(w_key.reshape(LATENT, H, NOPE), (1, 0, 2))
    value_maps = jnp.transpose(w_value.reshape(LATENT, H, VH), (1, 0, 2))
    key_index = jnp.arange(cached_all + tokens_all, dtype=jnp.int32)[None, :]
    row_index = jnp.arange(tokens_all, dtype=jnp.int32)[:, None]
    live_mask = jnp.where(key_index < cached_all, key_index < stretch_start, key_index - cached_all <= row_index)
    score_scale = 1.0 / math.sqrt(NOPE + ROPE)

    def one_head(operands):
        head_nope, head_rot, key_map, value_map = operands
        key_nope = jnp.dot(latent_all, key_map, preferred_element_type=jnp.float32).astype(jnp.bfloat16)
        value_rows = jnp.dot(latent_all, value_map, preferred_element_type=jnp.float32).astype(jnp.bfloat16)
        scores = jnp.dot(head_nope, key_nope.T, preferred_element_type=jnp.float32)
        scores = scores + jnp.dot(head_rot, key_rope.T, preferred_element_type=jnp.float32)
        scores = jnp.where(live_mask, scores * score_scale, -1e+30)
        top_score = lax.optimization_barrier(jnp.max(scores, axis=1, keepdims=True))
        exp_scores = jnp.exp(scores - top_score)
        weights = (exp_scores / lax.optimization_barrier(jnp.sum(exp_scores, axis=1, keepdims=True))).astype(jnp.bfloat16)
        return jnp.dot(weights, value_rows, preferred_element_type=jnp.float32).astype(jnp.bfloat16)
    outputs = lax.map(one_head, (query_nope, query_rot, key_maps, value_maps))
    return jnp.transpose(outputs, (1, 0, 2)).reshape(tokens_all, H * VH)
```

```python
import functools
import math

import jax
import jax.numpy as jnp
from jax import lax
from jax.experimental import pallas as pl
from jax.experimental.pallas import tpu as pltpu
from jax.sharding import Mesh
from jax.sharding import PartitionSpec as P

NOPE = 128
ROPE = 64
LATENT = 512
VH = 128
WIDE = 640
BLOCK = 512
AXES = ("gx", "px", "gy", "py", "z", "c")
GROUPS = ("gx", "px", "gy", "py")
SEQ = ("z", "c")
EPSILON = 1e-06
DEAD = -1e30
MESH = pl.DeviceIdType.MESH
NT = (((1,), (1,)), ((), ()))


def kernel(
    dims,
    q_hbm,
    rows_hbm,
    wk_hbm,
    wv_hbm,
    turn_ref,
    out_ref,
    w,
    keys,
    q,
    qs,
    scores,
    acc,
    top,
    total,
    local_sem,
    kr_s,
    kr_r,
    kc_s,
    kc_r,
    wr_s,
    wr_r,
    wx_s,
    wx_r,
    wc_s,
    wc_r,
):
    ring, tok, cache, heads = dims
    far = ring // 2
    z = lax.axis_index("z")
    c = lax.axis_index("c")
    px = lax.axis_index("px")
    py = lax.axis_index("py")
    rank = z * 2 + c
    cached_all = ring * 2 * cache
    half_rows = LATENT // 2
    up = {"z": lax.rem(z + 1, ring)}
    down = {"z": lax.rem(z + ring - 1, ring)}
    ways = (up, down)
    mate = {"c": 1 - c}
    sides = ({"px": 1 - px}, {"py": 1 - py})
    mine = (px, py)

    def far_slot(way, d):
        return lax.rem(z + ring - d, ring) if way == 0 else lax.rem(z + d, ring)

    def copy(src, dst, ssem, rsem, dev):
        return pltpu.make_async_remote_copy(
            src_ref=src, dst_ref=dst, send_sem=ssem, recv_sem=rsem, device_id=dev, device_id_type=MESH
        )

    barrier = pltpu.get_barrier_semaphore()
    for dev in (up, down, mate, *sides):
        pl.semaphore_signal(barrier, inc=1, device_id=dev, device_id_type=MESH)

    own_k = [
        pltpu.make_async_copy(
            rows_hbm.at[pl.ds(0, cache)], keys.at[pl.ds(rank * cache, cache)], local_sem.at[0]
        ),
        pltpu.make_async_copy(
            rows_hbm.at[pl.ds(cache, tok)],
            keys.at[pl.ds(cached_all + rank * tok, tok)],
            local_sem.at[1],
        ),
    ]
    own_w = [
        pltpu.make_async_copy(wk_hbm, w.at[rank, 0], local_sem.at[2]),
        pltpu.make_async_copy(wv_hbm, w.at[rank, 1], local_sem.at[3]),
    ]
    own_q = pltpu.make_async_copy(q_hbm, q, local_sem.at[4])
    for item in (*own_k, *own_w, own_q):
        item.start()
    pl.semaphore_wait(barrier, 5)

    def k_rows(zz, core, part):
        slot = zz * 2 + core
        if part == 0:
            return keys.at[pl.ds(slot * cache, cache)]
        return keys.at[pl.ds(cached_all + slot * tok, tok)]

    def k_ring(way, d, part):
        ref = k_rows(far_slot(way, d), c, part)
        return copy(ref, ref, kr_s.at[way, d, part], kr_r.at[way, d + 1, part], ways[way])

    def k_ring_in(way, d, part):
        ref = k_rows(far_slot(way, d), c, part)
        return copy(ref, ref, kr_s.at[way, d, part], kr_r.at[way, d, part], ways[way])

    def k_core(way, d, part):
        ref = k_rows(far_slot(way, d), c, part)
        return copy(ref, ref, kc_s.at[way, d, part], kc_r.at[way, d, part], mate)

    def k_core_in(way, d, part):
        ref = k_rows(far_slot(way, d), 1 - c, part)
        return copy(ref, ref, kc_s.at[way, d, part], kc_r.at[way, d, part], mate)

    def w_half(zz, core, m, half):
        return w.at[zz * 2 + core, m, pl.ds(half * half_rows, half_rows)]

    def w_ring(way, d, m):
        ref = w_half(far_slot(way, d), c, m, mine[m])
        return copy(ref, ref, wr_s.at[way, d, m], wr_r.at[way, d + 1, m], ways[way])

    def w_ring_in(way, d, m):
        ref = w_half(far_slot(way, d), c, m, mine[m])
        return copy(ref, ref, wr_s.at[way, d, m], wr_r.at[way, d, m], ways[way])

    def w_side(way, d, m):
        ref = w_half(far_slot(way, d), c, m, mine[m])
        return copy(ref, ref, wx_s.at[way, d, m], wx_r.at[way, d, m], sides[m])

    def w_side_in(way, d, m):
        ref = w_half(far_slot(way, d), c, m, 1 - mine[m])
        return copy(ref, ref, wx_s.at[way, d, m], wx_r.at[way, d, m], sides[m])

    def w_core(way, d, m):
        ref = w.at[far_slot(way, d) * 2 + c, m]
        return copy(ref, ref, wc_s.at[way, d, m], wc_r.at[way, d, m], mate)

    def w_core_in(way, d, m):
        ref = w.at[far_slot(way, d) * 2 + (1 - c), m]
        return copy(ref, ref, wc_s.at[way, d, m], wc_r.at[way, d, m], mate)

    for part in (0, 1):
        own_k[part].wait()
        k_ring(0, 0, part).start()
        k_ring(1, 0, part).start()
        k_core(0, 0, part).start()
    for m in (0, 1):
        own_w[m].wait()
        w_core(0, 0, m).start()

    def k_step(d, carry):
        for part in (0, 1):
            for way in (0, 1):
                k_ring_in(way, d, part).wait_recv()
                if carry is None:
                    k_ring(way, d, part).start()
                else:

                    @pl.when(jnp.logical_or(d < far - 1, part == way))
                    def _():
                        k_ring(way, d, part).start()

                k_core(way, d, part).start()
        return carry

    lax.fori_loop(1, far, k_step, 0)

    for m in (0, 1):
        for way in (0, 1):
            w_ring(way, 0, m).start()
    for part in (0, 1):
        k_ring_in(part, far, part).wait_recv()
        k_core(part, far, part).start()
    own_q.wait()

    lane = lax.broadcasted_iota(jnp.int32, (tok, ROPE), 1)
    ones_lane = jnp.where(lane == 0, 1.0, 0.0).astype(jnp.bfloat16)
    scale = math.log2(math.e) / math.sqrt(NOPE + ROPE)
    blocks = cached_all // BLOCK + (rank * tok) // BLOCK + 1
    rows_all = 2 * heads * tok

    def unit(zz, before_values):
        for core in (0, 1):
            slot = zz * 2 + core
            wide = heads * (NOPE + ROPE)
            block = q[:, pl.ds(pl.multiple_of(slot * wide, 128), wide)]
            for j in range(heads):
                at = j * (NOPE + ROPE)
                row = (core * heads + j) * tok
                lat = lax.dot_general(
                    block[:, at : at + NOPE],
                    w[slot, 0, :, j * NOPE : (j + 1) * NOPE],
                    NT,
                    preferred_element_type=jnp.float32,
                )
                qs[row : row + tok, :LATENT] = (lat * scale).astype(jnp.bfloat16)
                rot = block[:, at + NOPE : at + NOPE + ROPE].astype(jnp.float32)
                swapped = jnp.concatenate([rot[:, ROPE // 2 :], rot[:, : ROPE // 2]], 1)
                turned = (rot * turn_ref[:, :ROPE] + swapped * turn_ref[:, ROPE:]) * scale
                qs[row : row + tok, LATENT:] = jnp.concatenate(
                    [turned.astype(jnp.bfloat16), ones_lane], 1
                )

        def score(kb):
            first = pl.multiple_of(kb * BLOCK, BLOCK)
            return lax.dot_general(
                qs[...], keys[pl.ds(first, BLOCK), :], NT, preferred_element_type=jnp.float32
            )

        def lanes_max(s):
            best = s[:, :128]
            for n in range(1, BLOCK // 128):
                best = jnp.maximum(best, s[:, n * 128 : (n + 1) * 128])
            return best

        last = blocks - 1
        s = score(last)
        key_at = lax.broadcasted_iota(jnp.int32, (rows_all, BLOCK), 1)
        row_at = lax.rem(lax.broadcasted_iota(jnp.int32, (rows_all, BLOCK), 0), tok)
        edge = lax.rem(rank * tok, BLOCK)
        s = jnp.where(key_at <= row_at + edge, s, DEAD)
        scores[:, pl.ds(pl.multiple_of(last * BLOCK, BLOCK), BLOCK)] = s
        top[...] = lanes_max(s)

        def score_step(kb, carry):
            s = score(kb)
            scores[:, pl.ds(pl.multiple_of(kb * BLOCK, BLOCK), BLOCK)] = s
            top[...] = jnp.maximum(top[...], lanes_max(s))
            return carry

        lax.fori_loop(0, last, score_step, 0)
        best = jnp.max(top[...], axis=1, keepdims=True)
        top[...] = jnp.broadcast_to(best, top.shape)
        total[...] = jnp.zeros_like(total)
        acc[...] = jnp.zeros_like(acc)

        def value_step(kb, carry):
            first = pl.multiple_of(kb * BLOCK, BLOCK)
            parts = []
            best = top[...]
            run = total[...]
            for n in range(BLOCK // 128):
                p = jnp.exp2(scores[:, pl.ds(pl.multiple_of(first + n * 128, 128), 128)] - best)
                run = run + p
                parts.append(p.astype(jnp.bfloat16))
            total[...] = run
            weights = jnp.concatenate(parts, 1)
            acc[...] += jnp.dot(
                weights, keys[pl.ds(first, BLOCK), :LATENT], preferred_element_type=jnp.float32
            )
            return carry

        lax.fori_loop(0, blocks, value_step, 0)
        norm = 1.0 / jnp.sum(total[...], axis=1, keepdims=True)
        before_values()
        for core in (0, 1):
            slot = zz * 2 + core
            done = []
            for j in range(heads):
                row = (core * heads + j) * tok
                mixed = (acc[row : row + tok, :] * norm[row : row + tok]).astype(jnp.bfloat16)
                done.append(
                    jnp.dot(
                        mixed,
                        w[slot, 1, :, j * VH : (j + 1) * VH],
                        preferred_element_type=jnp.float32,
                    ).astype(jnp.bfloat16)
                )
            width = heads * VH
            out_ref[:, pl.ds(pl.multiple_of(slot * width, 128), width)] = jnp.concatenate(done, 1)

    def w_in(d, m, both=True):
        for way in (0, 1) if both else (m,):
            w_ring_in(way, d, m).wait_recv()
            if both:

                @pl.when(jnp.logical_or(d < far - 1, m == way))
                def _():
                    w_ring(way, d, m).start()

            w_side(way, d, m).start()

    def w_share(d, m, both=True):
        for way in (0, 1) if both else (m,):
            w_side_in(way, d, m).wait_recv()
            w_core(way, d, m).start()

    def waited_unit(way, e, value_way=None):
        w_core_in(way, e, 0).wait_recv()
        use = way if value_way is None else value_way
        unit(far_slot(way, e), lambda: w_core_in(use, e, 1).wait_recv())

    w_in(1, 0)
    for part in (0, 1):
        k_core_in(0, 0, part).wait_recv()

    def k_rest(d, carry):
        for part in (0, 1):
            for way in (0, 1):
                k_core_in(way, d, part).wait_recv()
        return carry

    lax.fori_loop(1, far, k_rest, 0)
    for part in (0, 1):
        k_core_in(part, far, part).wait_recv()
    w_in(1, 1)

    w_in(2, 0)
    w_share(1, 0)
    waited_unit(0, 0)
    w_in(2, 1)
    w_share(1, 1)

    def stage(d, carry):
        w_in(d, 0)
        w_share(d - 1, 0)
        waited_unit(0, d - 2)
        w_in(d, 1)
        w_share(d - 1, 1)
        waited_unit(1, d - 2)
        return carry

    lax.fori_loop(3, far, stage, 0)
    w_in(far, 0, False)
    w_share(far - 1, 0)
    waited_unit(0, far - 2)
    w_in(far, 1, False)
    w_share(far - 1, 1)
    w_share(far, 0, False)
    waited_unit(1, far - 2)
    w_share(far, 1, False)
    waited_unit(0, far - 1)
    waited_unit(1, far - 1)
    waited_unit(0, far, 1)

    for part in (0, 1):
        k_core(0, 0, part).wait_send()
        w_core(0, 0, part).wait_send()
        for way in (0, 1):
            k_ring(way, 0, part).wait_send()
            w_ring(way, 0, part).wait_send()

    def drain(d, carry):
        for part in (0, 1):
            for way in (0, 1):

                @pl.when(jnp.logical_or(d < far - 1, part == way))
                def _():
                    k_ring(way, d, part).wait_send()
                    w_ring(way, d, part).wait_send()

                k_core(way, d, part).wait_send()
                w_core(way, d, part).wait_send()
                w_side(way, d, part).wait_send()
        return carry

    lax.fori_loop(1, far, drain, 0)
    for part in (0, 1):
        k_core(part, far, part).wait_send()
        w_core(part, far, part).wait_send()
        w_side(part, far, part).wait_send()


def phases_for(positions, rope_width):
    half_width = rope_width // 2
    inverse = 10000.0 ** (-(jnp.arange(half_width, dtype=jnp.float32) * 2.0) / rope_width)
    return positions.astype(jnp.float32)[:, None] * inverse[None, :]


def local(queries, kv_new, kv_cache, kv_gain, w_key, w_value, prefix_len):
    ring = lax.axis_size("z")
    rank = lax.axis_index(SEQ)
    tok = queries.shape[0]
    cache = kv_cache.shape[0]
    heads = w_key.shape[1] // NOPE
    start = prefix_len[0]
    positions = start + rank * tok + jnp.arange(tok, dtype=jnp.int32)
    phases = phases_for(positions, ROPE)
    cosine, sine = jnp.cos(phases), jnp.sin(phases)
    turn = jnp.concatenate([cosine, cosine, -sine, sine], 1)
    raw = kv_new[:, :LATENT].astype(jnp.float32)
    inv_rms = lax.rsqrt(jnp.mean(raw * raw, axis=1, keepdims=True) + EPSILON)
    latent = (raw * inv_rms * kv_gain[None, :]).astype(jnp.bfloat16)
    rot = kv_new[:, LATENT:].astype(jnp.float32)
    swapped = jnp.concatenate([rot[:, ROPE // 2 :], rot[:, : ROPE // 2]], 1)
    rope = (rot * turn[:, :ROPE] + swapped * turn[:, ROPE:]).astype(jnp.bfloat16)
    pad = WIDE - LATENT - ROPE
    new_rows = jnp.concatenate([latent, rope, jnp.zeros((tok, pad), jnp.bfloat16)], 1)
    index = rank * cache + jnp.arange(cache, dtype=jnp.int32)[:, None]
    spare = jnp.arange(pad, dtype=jnp.int32)[None, :]
    bias = jnp.where((index >= start) & (spare == 0), DEAD, 0.0).astype(jnp.bfloat16)
    rows = jnp.concatenate([jnp.concatenate([kv_cache, bias], 1), new_rows], 0)
    slots = 2 * ring
    keys_all = slots * (cache + tok)
    rows_all = 2 * heads * tok
    hbm = pl.BlockSpec(memory_space=pl.ANY)
    vmem = pl.BlockSpec(memory_space=pltpu.VMEM)
    sems = pltpu.SemaphoreType.DMA((2, ring // 2 + 1, 2))
    out = pl.pallas_call(
        functools.partial(kernel, (ring, tok, cache, heads)),
        out_shape=jax.ShapeDtypeStruct((tok, slots * heads * VH), jnp.bfloat16),
        in_specs=[hbm, hbm, hbm, hbm, vmem],
        out_specs=vmem,
        scratch_shapes=[
            pltpu.VMEM((slots, 2, LATENT, heads * NOPE), jnp.bfloat16),
            pltpu.VMEM((keys_all, WIDE), jnp.bfloat16),
            pltpu.VMEM(queries.shape, jnp.bfloat16),
            pltpu.VMEM((rows_all, WIDE), jnp.bfloat16),
            pltpu.VMEM((rows_all, keys_all), jnp.float32),
            pltpu.VMEM((rows_all, LATENT), jnp.float32),
            pltpu.VMEM((rows_all, 128), jnp.float32),
            pltpu.VMEM((rows_all, 128), jnp.float32),
            pltpu.SemaphoreType.DMA((5,)),
        ]
        + [sems] * 10,
        compiler_params=pltpu.CompilerParams(
            collective_id=0, has_side_effects=True, vmem_limit_bytes=66 * 1000 * 1000
        ),
        name="attend",
    )(queries, rows, w_key, w_value, turn)
    return out


def solution(mesh):
    side = math.isqrt(mesh.shape["groups"])
    ring = mesh.shape["seq"] // 2
    torus = Mesh(mesh.devices.reshape(side // 2, 2, side // 2, 2, ring, 2), AXES)
    tokens = P((*GROUPS, *SEQ), None)
    placed = (tokens, tokens, tokens, P(), P(None, SEQ), P(None, SEQ), P(GROUPS))
    return jax.shard_map(local, mesh=torus, in_specs=placed, out_specs=tokens, check_vma=False)
```

```python
import functools
import math

import jax
import jax.numpy as jnp
from jax import lax
from jax.experimental import pallas as pl
from jax.experimental.pallas import tpu as pltpu
from jax.sharding import Mesh
from jax.sharding import PartitionSpec as P

NOPE = 128
ROPE = 64
LATENT = 512
VH = 128
WIDE = 640
BLOCK = 1024
LANES = 128
AXES = ("gx", "px", "gy", "py", "z", "c")
GROUPS = ("gx", "px", "gy", "py")
SEQ = ("z", "c")
EPSILON = 1e-06
DEAD = -1e30
MESH = pl.DeviceIdType.MESH
NT = (((1,), (1,)), ((), ()))


def kernel(
    dims,
    q_hbm,
    rows_hbm,
    wk_hbm,
    wv_hbm,
    turn_ref,
    out_hbm,
    w,
    keys,
    q,
    qs,
    scores,
    made,
    local_sem,
    ql_sem,
    ol_sem,
    q_s,
    q_r,
    o_s,
    o_r,
    kr_s,
    kr_r,
    kc_s,
    kc_r,
    wr_s,
    wr_r,
    wx_s,
    wx_r,
):
    ring, tok, cache, heads = dims
    far = ring // 2
    units = ring
    z = lax.axis_index("z")
    c = lax.axis_index("c")
    px = lax.axis_index("px")
    py = lax.axis_index("py")
    rank = z * 2 + c
    cached_all = ring * 2 * cache
    keys_all = cached_all + ring * 2 * tok
    chip = 2 * tok
    half_rows = LATENT // 2
    q_wide = heads * (NOPE + ROPE)
    o_wide = heads * VH
    up = {"z": lax.rem(z + 1, ring)}
    down = {"z": lax.rem(z + ring - 1, ring)}
    ways = (up, down)
    mate = {"c": 1 - c}
    sides = ({"px": 1 - px}, {"py": 1 - py})
    mine = (px, py)

    def far_slot(way, d):
        return lax.rem(z + ring + (2 * way - 1) * d, ring)

    def copy(src, dst, ssem, rsem, dev):
        return pltpu.make_async_remote_copy(
            src_ref=src, dst_ref=dst, send_sem=ssem, recv_sem=rsem, device_id=dev, device_id_type=MESH
        )

    barrier = pltpu.get_barrier_semaphore()
    for dev in (up, down, mate, *sides):
        pl.semaphore_signal(barrier, inc=1, device_id=dev, device_id_type=MESH)

    own_k = [
        pltpu.make_async_copy(
            rows_hbm.at[pl.ds(0, cache)], keys.at[pl.ds(rank * cache, cache)], local_sem.at[0]
        ),
        pltpu.make_async_copy(
            rows_hbm.at[pl.ds(cache, tok)],
            keys.at[pl.ds(cached_all + rank * tok, tok)],
            local_sem.at[1],
        ),
    ]
    own_w = [
        pltpu.make_async_copy(wk_hbm, w.at[z, 0], local_sem.at[2]),
        pltpu.make_async_copy(wv_hbm, w.at[z, 1], local_sem.at[3]),
    ]
    for item in (*own_k, *own_w):
        item.start()

    def q_from(zz, core):
        return q_hbm.at[:, pl.ds(pl.multiple_of((zz * 2 + core) * q_wide, LANES), q_wide)]

    def q_into(zz, core):
        return q.at[pl.ds(core * tok, tok), pl.ds(pl.multiple_of(zz * q_wide, LANES), q_wide)]

    def q_own(zz):
        return pltpu.make_async_copy(q_from(zz, c), q_into(zz, c), ql_sem.at[zz])

    def q_out(zz):
        return copy(q_from(zz, 1 - c), q_into(zz, c), q_s.at[zz], q_r.at[zz], mate)

    def q_in(zz):
        return copy(q_from(zz, c), q_into(zz, 1 - c), q_s.at[zz], q_r.at[zz], mate)

    def k_rows(zz, core, part):
        slot = zz * 2 + core
        if part == 0:
            return keys.at[pl.ds(slot * cache, cache)]
        return keys.at[pl.ds(cached_all + slot * tok, tok)]

    def k_ring(way, d, part):
        ref = k_rows(far_slot(way, d), c, part)
        return copy(ref, ref, kr_s.at[way, d, part], kr_r.at[way, d + 1, part], ways[way])

    def k_ring_in(way, d, part):
        ref = k_rows(far_slot(way, d), c, part)
        return copy(ref, ref, kr_s.at[way, d, part], kr_r.at[way, d, part], ways[way])

    def k_core(way, d, part):
        ref = k_rows(far_slot(way, d), c, part)
        return copy(ref, ref, kc_s.at[way, d, part], kc_r.at[way, d, part], mate)

    def k_core_in(way, d, part):
        ref = k_rows(far_slot(way, d), 1 - c, part)
        return copy(ref, ref, kc_s.at[way, d, part], kc_r.at[way, d, part], mate)

    def w_half(zz, m, half):
        return w.at[zz, m, pl.ds(half * half_rows, half_rows)]

    def w_ring(way, d, m):
        ref = w_half(far_slot(way, d), m, mine[m])
        return copy(ref, ref, wr_s.at[way, d, m], wr_r.at[way, d + 1, m], ways[way])

    def w_ring_in(way, d, m):
        ref = w_half(far_slot(way, d), m, mine[m])
        return copy(ref, ref, wr_s.at[way, d, m], wr_r.at[way, d, m], ways[way])

    def w_side(way, d, m):
        ref = w_half(far_slot(way, d), m, mine[m])
        return copy(ref, ref, wx_s.at[way, d, m], wx_r.at[way, d, m], sides[m])

    def w_side_in(way, d, m):
        ref = w_half(far_slot(way, d), m, 1 - mine[m])
        return copy(ref, ref, wx_s.at[way, d, m], wx_r.at[way, d, m], sides[m])

    slice_rows = half_rows // far

    def w_slice(way, n):
        ref = w.at[z, 0, pl.ds(mine[0] * half_rows + n * slice_rows, slice_rows)]
        return copy(ref, ref, wr_s.at[way, 0, 0], wr_r.at[way, 1, 0], ways[way])

    pl.semaphore_wait(barrier, 5)
    for part in (0, 1):
        own_k[part].wait()
        k_ring(0, 0, part).start()
        k_ring(1, 0, part).start()
        k_core(0, 0, part).start()
    own_w[0].wait()
    for way in (0, 1):
        w_slice(way, 0).start()

    def q_start(zz, carry):
        q_own(zz).start()
        q_out(zz).start()
        return carry

    lax.fori_loop(0, units, q_start, 0)

    def k_step(d, carry):
        for part in (0, 1):
            for way in (0, 1):
                k_ring_in(way, d, part).wait_recv()

                @pl.when(jnp.logical_or(d < far - 1, part == way))
                def _():
                    k_ring(way, d, part).start()

                k_core(way, d, part).start()
        for way in (0, 1):
            w_slice(way, d).start()
        return carry

    lax.fori_loop(1, far, k_step, 0)
    own_w[1].wait()
    for way in (0, 1):
        w_ring(way, 0, 1).start()
    for part in (0, 1):
        k_ring_in(part, far, part).wait_recv()
        k_core(part, far, part).start()

    def q_end(zz, carry):
        q_own(zz).wait()
        q_in(zz).wait_recv()
        return carry

    lax.fori_loop(0, units, q_end, 0)

    lane = lax.broadcasted_iota(jnp.int32, (chip, ROPE), 1)
    ones_lane = jnp.where(lane == 0, 1.0, 0.0).astype(jnp.bfloat16)
    scale = math.log2(math.e) / math.sqrt(NOPE + ROPE)

    def unit(zz, turn, before_values):
        block = q[:, pl.ds(pl.multiple_of(zz * q_wide, LANES), q_wide)]
        for j in range(heads):
            at = j * (NOPE + ROPE)
            row = j * chip
            lat = lax.dot_general(
                block[:, at : at + NOPE],
                w[zz, 0, :, j * NOPE : (j + 1) * NOPE],
                NT,
                preferred_element_type=jnp.float32,
            )
            qs[row : row + chip, :LATENT] = (lat * scale).astype(jnp.bfloat16)
            rot = block[:, at + NOPE : at + NOPE + ROPE].astype(jnp.float32)
            swapped = jnp.concatenate([rot[:, ROPE // 2 :], rot[:, : ROPE // 2]], 1)
            turned = (rot * turn_ref[:, :ROPE] + swapped * turn_ref[:, ROPE:]) * scale
            qs[row : row + chip, LATENT:] = jnp.concatenate(
                [turned.astype(jnp.bfloat16), ones_lane], 1
            )

        down_by = lax.broadcasted_iota(jnp.int32, (chip, LANES), 0) - lax.broadcasted_iota(
            jnp.int32, (chip, LANES), 1
        )
        down_by = jnp.concatenate([down_by] * heads, 0)
        best = None
        for first in range(0, keys_all, BLOCK):
            s = lax.dot_general(
                qs[...], keys[first : first + BLOCK, :], NT, preferred_element_type=jnp.float32
            )
            for n in range(0, BLOCK, LANES):
                tile = s[:, n : n + LANES]
                owner = (first + n - cached_all) // chip
                if owner >= 0:
                    tile = jnp.where(down_by >= (owner - z) * chip, tile, DEAD)
                scores[:, first + n : first + n + LANES] = tile
                best = tile if best is None else jnp.maximum(best, tile)
        best = jnp.broadcast_to(jnp.max(best, axis=1, keepdims=True), best.shape)
        total = None
        parts = []
        for first in range(0, keys_all, LANES):
            p = jnp.exp2(scores[:, first : first + LANES] - best)
            total = p if total is None else total + p
            parts.append(p.astype(jnp.bfloat16))
        acc = jnp.dot(
            jnp.concatenate(parts, 1), keys[:, :LATENT], preferred_element_type=jnp.float32
        )
        norm = 1.0 / jnp.sum(total, axis=1, keepdims=True)
        mixed = (acc * norm).astype(jnp.bfloat16)
        before_values()
        for j in range(heads):
            made[turn, :, j * VH : (j + 1) * VH] = jnp.dot(
                mixed[j * chip : (j + 1) * chip],
                w[zz, 1, :, j * VH : (j + 1) * VH],
                preferred_element_type=jnp.float32,
            ).astype(jnp.bfloat16)

    def w_in(d, m):
        for way in (0, 1):

            @pl.when(jnp.logical_or(d < far, m == way))
            def _():
                w_ring_in(way, d, m).wait_recv()

                @pl.when(jnp.logical_or(d < far - 1, jnp.logical_and(d < far, m == way)))
                def _():
                    w_ring(way, d, m).start()

                w_side(way, d, m).start()

    def chip_of(u):
        return far_slot(1 - lax.rem(u, 2), (u + 1) // 2)

    def o_into(u, core):
        slot = chip_of(u) * 2 + core
        return out_hbm.at[:, pl.ds(pl.multiple_of(slot * o_wide, LANES), o_wide)]

    def o_own(u):
        return pltpu.make_async_copy(
            made.at[u, pl.ds(c * tok, tok)], o_into(u, c), ol_sem.at[u]
        )

    def o_out(u):
        return copy(made.at[u, pl.ds((1 - c) * tok, tok)], o_into(u, c), o_s.at[u], o_r.at[u], mate)

    def o_in(u):
        return copy(made.at[u, pl.ds(c * tok, tok)], o_into(u, 1 - c), o_s.at[u], o_r.at[u], mate)

    for part in (0, 1):
        k_core_in(0, 0, part).wait_recv()

    def k_rest(d, carry):
        for part in (0, 1):
            for way in (0, 1):
                k_core_in(way, d, part).wait_recv()
        return carry

    lax.fori_loop(1, far, k_rest, 0)
    for part in (0, 1):
        k_core_in(part, far, part).wait_recv()
    w_in(1, 0)

    def step(u, carry):
        e = (u + 1) // 2
        odd = lax.rem(u, 2) == 1

        @pl.when(u == 1)
        def _():
            w_in(1, 1)

        for m in (0, 1):

            @pl.when(jnp.logical_and(odd == (m == 0), jnp.logical_and(u > 0, u < units - 1)))
            def _():
                w_in(e + 1, m)

        @pl.when(u > 0)
        def _():
            o_own(u - 1).start()
            o_out(u - 1).start()
            w_side_in(1 - lax.rem(u, 2), e, 0).wait_recv()

        def before_values():
            way = 1 - lax.rem(u, 2) + (u + 1) // units

            @pl.when(u > 0)
            def _():
                w_side_in(way, e, 1).wait_recv()

        unit(chip_of(u), u, before_values)
        return carry

    lax.fori_loop(0, units, step, 0)
    o_own(units - 1).start()
    o_out(units - 1).start()

    for part in (0, 1):
        k_core(0, 0, part).wait_send()
        for way in (0, 1):
            k_ring(way, 0, part).wait_send()
            w_ring(way, 0, part).wait_send()

    def drain(d, carry):
        for part in (0, 1):
            for way in (0, 1):

                @pl.when(jnp.logical_or(d < far - 1, part == way))
                def _():
                    k_ring(way, d, part).wait_send()
                    w_ring(way, d, part).wait_send()

                k_core(way, d, part).wait_send()
                w_side(way, d, part).wait_send()
        return carry

    lax.fori_loop(1, far, drain, 0)
    for part in (0, 1):
        k_core(part, far, part).wait_send()
        w_side(part, far, part).wait_send()

    def finish(u, carry):
        q_out(u).wait_send()
        o_own(u).wait()
        o_out(u).wait_send()
        o_in(u).wait_recv()
        return carry

    lax.fori_loop(0, units, finish, 0)


def phases_for(positions, rope_width):
    half_width = rope_width // 2
    inverse = 10000.0 ** (-(jnp.arange(half_width, dtype=jnp.float32) * 2.0) / rope_width)
    return positions.astype(jnp.float32)[:, None] * inverse[None, :]


def local(queries, kv_new, kv_cache, kv_gain, w_key, w_value, prefix_len):
    ring = lax.axis_size("z")
    rank = lax.axis_index(SEQ)
    tok = queries.shape[0]
    cache = kv_cache.shape[0]
    heads = w_key.shape[1] // NOPE
    start = prefix_len[0]
    base = start + lax.axis_index("z") * (2 * tok)
    phases = phases_for(base + jnp.arange(2 * tok, dtype=jnp.int32), ROPE)
    cosine, sine = jnp.cos(phases), jnp.sin(phases)
    turns = jnp.concatenate([cosine, cosine, -sine, sine], 1)
    turn = lax.dynamic_slice_in_dim(turns, lax.axis_index("c") * tok, tok, 0)
    raw = kv_new[:, :LATENT].astype(jnp.float32)
    inv_rms = lax.rsqrt(jnp.mean(raw * raw, axis=1, keepdims=True) + EPSILON)
    latent = (raw * inv_rms * kv_gain[None, :]).astype(jnp.bfloat16)
    rot = kv_new[:, LATENT:].astype(jnp.float32)
    swapped = jnp.concatenate([rot[:, ROPE // 2 :], rot[:, : ROPE // 2]], 1)
    rope = (rot * turn[:, :ROPE] + swapped * turn[:, ROPE:]).astype(jnp.bfloat16)
    pad = WIDE - LATENT - ROPE
    new_rows = jnp.concatenate([latent, rope, jnp.zeros((tok, pad), jnp.bfloat16)], 1)
    index = rank * cache + jnp.arange(cache, dtype=jnp.int32)[:, None]
    spare = jnp.arange(pad, dtype=jnp.int32)[None, :]
    bias = jnp.where((index >= start) & (spare == 0), DEAD, 0.0).astype(jnp.bfloat16)
    rows = jnp.concatenate([jnp.concatenate([kv_cache, bias], 1), new_rows], 0)
    slots = 2 * ring
    keys_all = slots * (cache + tok)
    rows_all = 2 * heads * tok
    hbm = pl.BlockSpec(memory_space=pl.ANY)
    vmem = pl.BlockSpec(memory_space=pltpu.VMEM)
    each = pltpu.SemaphoreType.DMA((ring,))
    sems = pltpu.SemaphoreType.DMA((2, ring // 2 + 1, 2))
    return pl.pallas_call(
        functools.partial(kernel, (ring, tok, cache, heads)),
        out_shape=jax.ShapeDtypeStruct((tok, slots * heads * VH), jnp.bfloat16),
        in_specs=[hbm, hbm, hbm, hbm, vmem],
        out_specs=hbm,
        scratch_shapes=[
            pltpu.VMEM((ring, 2, LATENT, heads * NOPE), jnp.bfloat16),
            pltpu.VMEM((keys_all, WIDE), jnp.bfloat16),
            pltpu.VMEM((2 * tok, ring * heads * (NOPE + ROPE)), jnp.bfloat16),
            pltpu.VMEM((rows_all, WIDE), jnp.bfloat16),
            pltpu.VMEM((rows_all, keys_all), jnp.float32),
            pltpu.VMEM((ring, 2 * tok, heads * VH), jnp.bfloat16),
            pltpu.SemaphoreType.DMA((4,)),
        ]
        + [each] * 6
        + [sems] * 8,
        compiler_params=pltpu.CompilerParams(
            collective_id=0, has_side_effects=True, vmem_limit_bytes=66 * 1000 * 1000
        ),
        name="attend",
    )(queries, rows, w_key, w_value, turns)


def solution(mesh):
    side = math.isqrt(mesh.shape["groups"])
    ring = mesh.shape["seq"] // 2
    torus = Mesh(mesh.devices.reshape(side // 2, 2, side // 2, 2, ring, 2), AXES)
    tokens = P((*GROUPS, *SEQ), None)
    placed = (tokens, tokens, tokens, P(), P(None, SEQ), P(None, SEQ), P(GROUPS))
    return jax.shard_map(local, mesh=torus, in_specs=placed, out_specs=tokens, check_vma=False)
```

```python
import functools
import math

import jax
import jax.numpy as jnp
from jax import lax
from jax.experimental import pallas as pl
from jax.experimental.pallas import tpu as pltpu
from jax.sharding import Mesh
from jax.sharding import PartitionSpec as P

NOPE = 128
ROPE = 64
LATENT = 512
VH = 128
WIDE = 640
BLOCK = 1024
LANES = 128
AXES = ("gx", "px", "gy", "py", "z", "c")
GROUPS = ("gx", "px", "gy", "py")
SEQ = ("z", "c")
EPSILON = 1e-06
DEAD = -1e30
MESH = pl.DeviceIdType.MESH
NT = (((1,), (1,)), ((), ()))


def kernel(
    dims,
    start_ref,
    q_hbm,
    new_ref,
    cache_ref,
    gain_ref,
    wk_hbm,
    wv_hbm,
    out_hbm,
    w,
    keys,
    q,
    turn_ref,
    qs,
    scores,
    made,
    local_sem,
    ql_sem,
    ol_sem,
    q_s,
    q_r,
    o_s,
    o_r,
    kr_s,
    kr_r,
    kc_s,
    kc_r,
    wr_s,
    wr_r,
    wx_s,
    wx_r,
):
    ring, tok, cache, heads = dims
    far = ring // 2
    units = ring
    z = lax.axis_index("z")
    c = lax.axis_index("c")
    px = lax.axis_index("px")
    py = lax.axis_index("py")
    rank = z * 2 + c
    cached_all = ring * 2 * cache
    keys_all = cached_all + ring * 2 * tok
    chip = 2 * tok
    half_rows = LATENT // 2
    q_wide = heads * (NOPE + ROPE)
    o_wide = heads * VH
    up = {"z": lax.rem(z + 1, ring)}
    down = {"z": lax.rem(z + ring - 1, ring)}
    ways = (up, down)
    mate = {"c": 1 - c}
    sides = ({"px": 1 - px}, {"py": 1 - py})
    mine = (px, py)

    def far_slot(way, d):
        return lax.rem(z + ring + (2 * way - 1) * d, ring)

    def copy(src, dst, ssem, rsem, dev):
        return pltpu.make_async_remote_copy(
            src_ref=src, dst_ref=dst, send_sem=ssem, recv_sem=rsem, device_id=dev, device_id_type=MESH
        )

    barrier = pltpu.get_barrier_semaphore()
    for dev in (up, down, mate, *sides):
        pl.semaphore_signal(barrier, inc=1, device_id=dev, device_id_type=MESH)

    own_w = [
        pltpu.make_async_copy(wk_hbm, w.at[z, 0], local_sem.at[0]),
        pltpu.make_async_copy(wv_hbm, w.at[z, 1], local_sem.at[1]),
    ]
    for item in own_w:
        item.start()

    def q_from(zz, core):
        return q_hbm.at[:, pl.ds(pl.multiple_of((zz * 2 + core) * q_wide, LANES), q_wide)]

    def q_into(zz, core):
        return q.at[pl.ds(core * tok, tok), pl.ds(pl.multiple_of(zz * q_wide, LANES), q_wide)]

    def q_own(zz):
        return pltpu.make_async_copy(q_from(zz, c), q_into(zz, c), ql_sem.at[zz])

    def q_out(zz):
        return copy(q_from(zz, 1 - c), q_into(zz, c), q_s.at[zz], q_r.at[zz], mate)

    def q_in(zz):
        return copy(q_from(zz, c), q_into(zz, 1 - c), q_s.at[zz], q_r.at[zz], mate)

    def k_rows(zz, core, part):
        slot = zz * 2 + core
        if part == 0:
            return keys.at[pl.ds(slot * cache, cache)]
        return keys.at[pl.ds(cached_all + slot * tok, tok)]

    def k_ring(way, d, part):
        ref = k_rows(far_slot(way, d), c, part)
        return copy(ref, ref, kr_s.at[way, d, part], kr_r.at[way, d + 1, part], ways[way])

    def k_ring_in(way, d, part):
        ref = k_rows(far_slot(way, d), c, part)
        return copy(ref, ref, kr_s.at[way, d, part], kr_r.at[way, d, part], ways[way])

    def k_core(way, d, part):
        ref = k_rows(far_slot(way, d), c, part)
        return copy(ref, ref, kc_s.at[way, d, part], kc_r.at[way, d, part], mate)

    def k_core_in(way, d, part):
        ref = k_rows(far_slot(way, d), 1 - c, part)
        return copy(ref, ref, kc_s.at[way, d, part], kc_r.at[way, d, part], mate)

    def w_half(zz, m, half):
        return w.at[zz, m, pl.ds(half * half_rows, half_rows)]

    def w_ring(way, d, m):
        ref = w_half(far_slot(way, d), m, mine[m])
        return copy(ref, ref, wr_s.at[way, d, m], wr_r.at[way, d + 1, m], ways[way])

    def w_ring_in(way, d, m):
        ref = w_half(far_slot(way, d), m, mine[m])
        return copy(ref, ref, wr_s.at[way, d, m], wr_r.at[way, d, m], ways[way])

    def w_side(way, d, m):
        ref = w_half(far_slot(way, d), m, mine[m])
        return copy(ref, ref, wx_s.at[way, d, m], wx_r.at[way, d, m], sides[m])

    def w_side_in(way, d, m):
        ref = w_half(far_slot(way, d), m, 1 - mine[m])
        return copy(ref, ref, wx_s.at[way, d, m], wx_r.at[way, d, m], sides[m])

    slice_rows = 2 * half_rows // far

    def w_slice(way, m, n):
        ref = w.at[z, m, pl.ds(mine[m] * half_rows + n * slice_rows, slice_rows)]
        return copy(ref, ref, wr_s.at[way, 0, m], wr_r.at[way, 1, m], ways[way])

    begin = start_ref[0]
    half = ROPE // 2
    wave = lax.broadcasted_iota(jnp.int32, (chip, LANES), 1)
    inverse = jnp.exp(lax.rem(wave, half).astype(jnp.float32) * (-2.0 * math.log(10000.0) / ROPE))
    place = begin + z * chip + lax.broadcasted_iota(jnp.int32, (chip, LANES), 0)
    phases = place.astype(jnp.float32) * inverse
    sine = jnp.sin(phases)
    turn_ref[...] = jnp.where(
        wave < ROPE, jnp.cos(phases), jnp.where(wave < ROPE + half, -sine, sine)
    )
    raw = new_ref[:, :LATENT].astype(jnp.float32)
    inv_rms = lax.rsqrt(jnp.mean(raw * raw, axis=1, keepdims=True) + EPSILON)
    new_at = pl.ds(pl.multiple_of(cached_all + rank * tok, tok), tok)
    keys[new_at, :LATENT] = (raw * inv_rms * gain_ref[...]).astype(jnp.bfloat16)
    rot = new_ref[:, LATENT:].astype(jnp.float32)
    swapped = jnp.concatenate([rot[:, half:], rot[:, :half]], 1)
    turn_own = turn_ref[pl.ds(pl.multiple_of(c * tok, tok), tok), :]
    rope_new = (rot * turn_own[:, :ROPE] + swapped * turn_own[:, ROPE:]).astype(jnp.bfloat16)
    pad = WIDE - LATENT - ROPE
    keys[new_at, LATENT:] = jnp.concatenate([rope_new, jnp.zeros((tok, pad), jnp.bfloat16)], 1)
    cache_at = pl.ds(pl.multiple_of(rank * cache, cache), cache)
    keys[cache_at, :LATENT] = cache_ref[:, :LATENT]
    spare = lax.broadcasted_iota(jnp.int32, (cache, pad), 1)
    index = rank * cache + lax.broadcasted_iota(jnp.int32, (cache, pad), 0)
    bias = jnp.where(jnp.logical_and(index >= begin, spare == 0), DEAD, 0.0).astype(jnp.bfloat16)
    keys[cache_at, LATENT:] = jnp.concatenate([cache_ref[:, LATENT:], bias], 1)

    pl.semaphore_wait(barrier, 5)
    for part in (0, 1):
        k_ring(0, 0, part).start()
        k_ring(1, 0, part).start()
        k_core(0, 0, part).start()
    for m in (0, 1):
        own_w[m].wait()
    for way in (0, 1):
        w_slice(way, 0, 0).start()

    def q_start(zz, carry):
        q_own(zz).start()
        q_out(zz).start()
        return carry

    lax.fori_loop(0, units, q_start, 0)

    def k_step(d, carry):
        for part in (0, 1):
            for way in (0, 1):
                k_ring_in(way, d, part).wait_recv()

                @pl.when(jnp.logical_or(d < far - 1, part == way))
                def _():
                    k_ring(way, d, part).start()

                k_core(way, d, part).start()
        for m in (0, 1):

            @pl.when(d // (far // 2) == m)
            def _():
                for way in (0, 1):
                    w_slice(way, m, d - m * (far // 2)).start()

        @pl.when(d == far - 2)
        def _():
            for way in (0, 1):
                w_ring_in(way, 1, 0).wait_recv()
                w_side(way, 1, 0).start()

        return carry

    lax.fori_loop(1, far, k_step, 0)
    for way in (0, 1):
        w_ring(way, 1, 0).start()
    for part in (0, 1):
        k_ring_in(part, far, part).wait_recv()
        k_core(part, far, part).start()

    def q_end(zz, carry):
        q_own(zz).wait()
        q_in(zz).wait_recv()
        return carry

    lax.fori_loop(0, units, q_end, 0)

    lane = lax.broadcasted_iota(jnp.int32, (chip, ROPE), 1)
    ones_lane = jnp.where(lane == 0, 1.0, 0.0).astype(jnp.bfloat16)
    scale = math.log2(math.e) / math.sqrt(NOPE + ROPE)

    def unit(zz, turn, before_values):
        block = q[:, pl.ds(pl.multiple_of(zz * q_wide, LANES), q_wide)]
        for j in range(heads):
            at = j * (NOPE + ROPE)
            row = j * chip
            lat = lax.dot_general(
                block[:, at : at + NOPE],
                w[zz, 0, :, j * NOPE : (j + 1) * NOPE],
                NT,
                preferred_element_type=jnp.float32,
            )
            qs[row : row + chip, :LATENT] = (lat * scale).astype(jnp.bfloat16)
            rot = block[:, at + NOPE : at + NOPE + ROPE].astype(jnp.float32)
            swapped = jnp.concatenate([rot[:, ROPE // 2 :], rot[:, : ROPE // 2]], 1)
            turned = (rot * turn_ref[:, :ROPE] + swapped * turn_ref[:, ROPE:]) * scale
            qs[row : row + chip, LATENT:] = jnp.concatenate(
                [turned.astype(jnp.bfloat16), ones_lane], 1
            )

        down_by = lax.broadcasted_iota(jnp.int32, (chip, LANES), 0) - lax.broadcasted_iota(
            jnp.int32, (chip, LANES), 1
        )
        down_by = jnp.concatenate([down_by] * heads, 0)
        best = None
        for first in range(0, keys_all, BLOCK):
            s = lax.dot_general(
                qs[...], keys[first : first + BLOCK, :], NT, preferred_element_type=jnp.float32
            )
            for n in range(0, BLOCK, LANES):
                tile = s[:, n : n + LANES]
                owner = (first + n - cached_all) // chip
                if owner >= 0:
                    tile = jnp.where(down_by >= (owner - z) * chip, tile, DEAD)
                scores[:, first + n : first + n + LANES] = tile
                best = tile if best is None else jnp.maximum(best, tile)
        best = jnp.broadcast_to(jnp.max(best, axis=1, keepdims=True), best.shape)
        total = None
        parts = []
        for first in range(0, keys_all, LANES):
            p = jnp.exp2(scores[:, first : first + LANES] - best)
            total = p if total is None else total + p
            parts.append(p.astype(jnp.bfloat16))
        acc = jnp.dot(
            jnp.concatenate(parts, 1), keys[:, :LATENT], preferred_element_type=jnp.float32
        )
        norm = 1.0 / jnp.sum(total, axis=1, keepdims=True)
        mixed = (acc * norm).astype(jnp.bfloat16)
        before_values()
        for j in range(heads):
            made[turn, :, j * VH : (j + 1) * VH] = jnp.dot(
                mixed[j * chip : (j + 1) * chip],
                w[zz, 1, :, j * VH : (j + 1) * VH],
                preferred_element_type=jnp.float32,
            ).astype(jnp.bfloat16)

    def w_in(d, m):
        for way in (0, 1):

            @pl.when(jnp.logical_or(d < far, m == way))
            def _():
                w_ring_in(way, d, m).wait_recv()

                @pl.when(jnp.logical_or(d < far - 1, jnp.logical_and(d < far, m == way)))
                def _():
                    w_ring(way, d, m).start()

                w_side(way, d, m).start()

    def chip_of(u):
        return far_slot(1 - lax.rem(u, 2), (u + 1) // 2)

    def o_into(u, core):
        slot = chip_of(u) * 2 + core
        return out_hbm.at[:, pl.ds(pl.multiple_of(slot * o_wide, LANES), o_wide)]

    def o_own(u):
        return pltpu.make_async_copy(
            made.at[u, pl.ds(c * tok, tok)], o_into(u, c), ol_sem.at[u]
        )

    def o_out(u):
        return copy(made.at[u, pl.ds((1 - c) * tok, tok)], o_into(u, c), o_s.at[u], o_r.at[u], mate)

    def o_in(u):
        return copy(made.at[u, pl.ds(c * tok, tok)], o_into(u, 1 - c), o_s.at[u], o_r.at[u], mate)

    for part in (0, 1):
        k_core_in(0, 0, part).wait_recv()

    def k_rest(d, carry):
        for part in (0, 1):
            for way in (0, 1):
                k_core_in(way, d, part).wait_recv()
        return carry

    lax.fori_loop(1, far, k_rest, 0)
    for part in (0, 1):
        k_core_in(part, far, part).wait_recv()

    def step(u, carry):
        e = (u + 1) // 2
        odd = lax.rem(u, 2) == 1

        @pl.when(u == 1)
        def _():
            w_in(1, 1)

        for m in (0, 1):

            @pl.when(jnp.logical_and(odd == (m == 0), jnp.logical_and(u > 0, u < units - 1)))
            def _():
                w_in(e + 1, m)

        @pl.when(u > 0)
        def _():
            o_own(u - 1).start()
            o_out(u - 1).start()
            w_side_in(1 - lax.rem(u, 2), e, 0).wait_recv()

        def before_values():
            way = 1 - lax.rem(u, 2) + (u + 1) // units

            @pl.when(u > 0)
            def _():
                w_side_in(way, e, 1).wait_recv()

        unit(chip_of(u), u, before_values)
        return carry

    lax.fori_loop(0, units, step, 0)
    o_own(units - 1).start()
    o_out(units - 1).start()

    for part in (0, 1):
        k_core(0, 0, part).wait_send()
        for way in (0, 1):
            k_ring(way, 0, part).wait_send()
            w_ring(way, 0, part).wait_send()

    def drain(d, carry):
        for part in (0, 1):
            for way in (0, 1):

                @pl.when(jnp.logical_or(d < far - 1, part == way))
                def _():
                    k_ring(way, d, part).wait_send()
                    w_ring(way, d, part).wait_send()

                k_core(way, d, part).wait_send()
                w_side(way, d, part).wait_send()
        return carry

    lax.fori_loop(1, far, drain, 0)
    for part in (0, 1):
        k_core(part, far, part).wait_send()
        w_side(part, far, part).wait_send()

    def finish(u, carry):
        q_out(u).wait_send()
        o_own(u).wait()
        o_out(u).wait_send()
        o_in(u).wait_recv()
        return carry

    lax.fori_loop(0, units, finish, 0)


def local(queries, kv_new, kv_cache, kv_gain, w_key, w_value, prefix_len):
    ring = lax.axis_size("z")
    tok = queries.shape[0]
    cache = kv_cache.shape[0]
    heads = w_key.shape[1] // NOPE
    slots = 2 * ring
    keys_all = slots * (cache + tok)
    rows_all = 2 * heads * tok
    hbm = pl.BlockSpec(memory_space=pl.ANY)
    vmem = pl.BlockSpec(memory_space=pltpu.VMEM)
    each = pltpu.SemaphoreType.DMA((ring,))
    sems = pltpu.SemaphoreType.DMA((2, ring // 2 + 1, 2))
    return pl.pallas_call(
        functools.partial(kernel, (ring, tok, cache, heads)),
        out_shape=jax.ShapeDtypeStruct((tok, slots * heads * VH), jnp.bfloat16),
        in_specs=[
            pl.BlockSpec(memory_space=pltpu.SMEM),
            hbm,
            vmem,
            vmem,
            vmem,
            hbm,
            hbm,
        ],
        out_specs=hbm,
        scratch_shapes=[
            pltpu.VMEM((ring, 2, LATENT, heads * NOPE), jnp.bfloat16),
            pltpu.VMEM((keys_all, WIDE), jnp.bfloat16),
            pltpu.VMEM((2 * tok, ring * heads * (NOPE + ROPE)), jnp.bfloat16),
            pltpu.VMEM((2 * tok, LANES), jnp.float32),
            pltpu.VMEM((rows_all, WIDE), jnp.bfloat16),
            pltpu.VMEM((rows_all, keys_all), jnp.float32),
            pltpu.VMEM((ring, 2 * tok, heads * VH), jnp.bfloat16),
            pltpu.SemaphoreType.DMA((2,)),
        ]
        + [each] * 6
        + [sems] * 8,
        compiler_params=pltpu.CompilerParams(
            collective_id=0, has_side_effects=True, vmem_limit_bytes=66 * 1000 * 1000
        ),
        name="attend",
    )(prefix_len, queries, kv_new, kv_cache, kv_gain[None, :], w_key, w_value)


def solution(mesh):
    side = math.isqrt(mesh.shape["groups"])
    ring = mesh.shape["seq"] // 2
    torus = Mesh(mesh.devices.reshape(side // 2, 2, side // 2, 2, ring, 2), AXES)
    tokens = P((*GROUPS, *SEQ), None)
    placed = (tokens, tokens, tokens, P(), P(None, SEQ), P(None, SEQ), P(GROUPS))
    return jax.shard_map(local, mesh=torus, in_specs=placed, out_specs=tokens, check_vma=False)
```

```python
import functools
import math

import jax
import jax.numpy as jnp
from jax import lax
from jax.experimental import pallas as pl
from jax.experimental.pallas import tpu as pltpu
from jax.sharding import Mesh
from jax.sharding import PartitionSpec as P

NOPE = 128
ROPE = 64
LATENT = 512
VH = 128
WIDE = 640
BLOCK = 1024
LANES = 128
PARTS = (0, 1, 2)
AXES = ("gx", "px", "gy", "py", "z", "c")
GROUPS = ("gx", "px", "gy", "py")
SEQ = ("z", "c")
EPSILON = 1e-06
DEAD = -1e30
MESH = pl.DeviceIdType.MESH
NT = (((1,), (1,)), ((), ()))


def kernel(
    dims,
    start_ref,
    q_hbm,
    new_ref,
    cache_ref,
    gain_ref,
    wk_hbm,
    wv_hbm,
    out_hbm,
    w,
    keys,
    q,
    turn_ref,
    qs,
    scores,
    mixed,
    made,
    local_sem,
    ql_sem,
    ol_sem,
    q_s,
    q_r,
    o_s,
    o_r,
    kr_s,
    kr_r,
    kc_s,
    kc_r,
    wr_s,
    wr_r,
    wx_s,
    wx_r,
):
    ring, tok, cache, heads = dims
    far = ring // 2
    units = ring
    z = lax.axis_index("z")
    c = lax.axis_index("c")
    px = lax.axis_index("px")
    py = lax.axis_index("py")
    rank = z * 2 + c
    cached_all = ring * 2 * cache
    keys_all = cached_all + ring * 2 * tok
    chip = 2 * tok
    half_rows = LATENT // 2
    q_wide = heads * (NOPE + ROPE)
    o_wide = heads * VH
    up = {"z": lax.rem(z + 1, ring)}
    down = {"z": lax.rem(z + ring - 1, ring)}
    ways = (up, down)
    mate = {"c": 1 - c}
    sides = ({"px": 1 - px}, {"py": 1 - py})
    mine = (px, py)

    def far_slot(way, d):
        return lax.rem(z + ring + (2 * way - 1) * d, ring)

    def copy(src, dst, ssem, rsem, dev):
        return pltpu.make_async_remote_copy(
            src_ref=src, dst_ref=dst, send_sem=ssem, recv_sem=rsem, device_id=dev, device_id_type=MESH
        )

    barrier = pltpu.get_barrier_semaphore()
    for dev in (up, down, mate, *sides):
        pl.semaphore_signal(barrier, inc=1, device_id=dev, device_id_type=MESH)

    own_w = [
        pltpu.make_async_copy(wk_hbm, w.at[z, 0], local_sem.at[0]),
        pltpu.make_async_copy(wv_hbm, w.at[z, 1], local_sem.at[1]),
    ]
    for item in own_w:
        item.start()

    def q_from(zz, core):
        return q_hbm.at[:, pl.ds(pl.multiple_of((zz * 2 + core) * q_wide, LANES), q_wide)]

    def q_into(zz, core):
        return q.at[pl.ds(core * tok, tok), pl.ds(pl.multiple_of(zz * q_wide, LANES), q_wide)]

    def q_own(zz):
        return pltpu.make_async_copy(q_from(zz, c), q_into(zz, c), ql_sem.at[zz])

    def q_out(zz):
        return copy(q_from(zz, 1 - c), q_into(zz, c), q_s.at[zz], q_r.at[zz], mate)

    def q_in(zz):
        return copy(q_from(zz, c), q_into(zz, 1 - c), q_s.at[zz], q_r.at[zz], mate)

    def k_rows(zz, core, part):
        slot = zz * 2 + core
        if part == 0:
            return keys.at[pl.ds(slot * cache, cache)]
        return keys.at[pl.ds(cached_all + slot * tok + (part - 1) * (tok // 2), tok // 2)]

    def k_ring(way, d, part):
        ref = k_rows(far_slot(way, d), c, part)
        return copy(ref, ref, kr_s.at[way, d, part], kr_r.at[way, d + 1, part], ways[way])

    def k_ring_in(way, d, part):
        ref = k_rows(far_slot(way, d), c, part)
        return copy(ref, ref, kr_s.at[way, d, part], kr_r.at[way, d, part], ways[way])

    def k_core(way, d, part):
        ref = k_rows(far_slot(way, d), c, part)
        return copy(ref, ref, kc_s.at[way, d, part], kc_r.at[way, d, part], mate)

    def k_core_in(way, d, part):
        ref = k_rows(far_slot(way, d), 1 - c, part)
        return copy(ref, ref, kc_s.at[way, d, part], kc_r.at[way, d, part], mate)

    def w_half(zz, m, half):
        return w.at[zz, m, pl.ds(half * half_rows, half_rows)]

    def w_ring(way, d, m):
        ref = w_half(far_slot(way, d), m, mine[m])
        return copy(ref, ref, wr_s.at[way, d, m], wr_r.at[way, d + 1, m], ways[way])

    def w_ring_in(way, d, m):
        ref = w_half(far_slot(way, d), m, mine[m])
        return copy(ref, ref, wr_s.at[way, d, m], wr_r.at[way, d, m], ways[way])

    def w_side(way, d, m):
        ref = w_half(far_slot(way, d), m, mine[m])
        return copy(ref, ref, wx_s.at[way, d, m], wx_r.at[way, d, m], sides[m])

    def w_side_in(way, d, m):
        ref = w_half(far_slot(way, d), m, 1 - mine[m])
        return copy(ref, ref, wx_s.at[way, d, m], wx_r.at[way, d, m], sides[m])

    slice_rows = 2 * half_rows // far

    def w_slice(way, m, n):
        ref = w.at[z, m, pl.ds(mine[m] * half_rows + n * slice_rows, slice_rows)]
        return copy(ref, ref, wr_s.at[way, 0, m], wr_r.at[way, 1, m], ways[way])

    begin = start_ref[0]
    half = ROPE // 2
    wave = lax.broadcasted_iota(jnp.int32, (chip, LANES), 1)
    inverse = jnp.exp(lax.rem(wave, half).astype(jnp.float32) * (-2.0 * math.log(10000.0) / ROPE))
    place = begin + z * chip + lax.broadcasted_iota(jnp.int32, (chip, LANES), 0)
    phases = place.astype(jnp.float32) * inverse
    sine = jnp.sin(phases)
    turn_ref[...] = jnp.where(
        wave < ROPE, jnp.cos(phases), jnp.where(wave < ROPE + half, -sine, sine)
    )
    raw = new_ref[:, :LATENT].astype(jnp.float32)
    inv_rms = lax.rsqrt(jnp.mean(raw * raw, axis=1, keepdims=True) + EPSILON)
    new_at = pl.ds(pl.multiple_of(cached_all + rank * tok, tok), tok)
    keys[new_at, :LATENT] = (raw * inv_rms * gain_ref[...]).astype(jnp.bfloat16)
    rot = new_ref[:, LATENT:].astype(jnp.float32)
    swapped = jnp.concatenate([rot[:, half:], rot[:, :half]], 1)
    turn_own = turn_ref[pl.ds(pl.multiple_of(c * tok, tok), tok), :]
    rope_new = (rot * turn_own[:, :ROPE] + swapped * turn_own[:, ROPE:]).astype(jnp.bfloat16)
    pad = WIDE - LATENT - ROPE
    keys[new_at, LATENT:] = jnp.concatenate([rope_new, jnp.zeros((tok, pad), jnp.bfloat16)], 1)
    cache_at = pl.ds(pl.multiple_of(rank * cache, cache), cache)
    keys[cache_at, :LATENT] = cache_ref[:, :LATENT]
    spare = lax.broadcasted_iota(jnp.int32, (cache, pad), 1)
    index = rank * cache + lax.broadcasted_iota(jnp.int32, (cache, pad), 0)
    bias = jnp.where(jnp.logical_and(index >= begin, spare == 0), DEAD, 0.0).astype(jnp.bfloat16)
    keys[cache_at, LATENT:] = jnp.concatenate([cache_ref[:, LATENT:], bias], 1)

    pl.semaphore_wait(barrier, 5)
    for part in PARTS:
        k_ring(0, 0, part).start()
        k_ring(1, 0, part).start()
        k_core(0, 0, part).start()
    for m in (0, 1):
        own_w[m].wait()
    for way in (0, 1):
        w_slice(way, 0, 0).start()

    def q_start(zz, carry):
        q_own(zz).start()
        q_out(zz).start()
        return carry

    lax.fori_loop(0, units, q_start, 0)

    def k_step(d, carry):
        for part in PARTS:
            for way in (0, 1):
                k_ring_in(way, d, part).wait_recv()

                @pl.when(jnp.logical_or(d < far - 1, part % 2 == way))
                def _():
                    k_ring(way, d, part).start()

                k_core(way, d, part).start()
        for m in (0, 1):

            @pl.when(d // (far // 2) == m)
            def _():
                for way in (0, 1):
                    w_slice(way, m, d - m * (far // 2)).start()

        @pl.when(d == far - 2)
        def _():
            for way in (0, 1):
                w_ring_in(way, 1, 0).wait_recv()
                w_side(way, 1, 0).start()

        return carry

    lax.fori_loop(1, far, k_step, 0)
    for way in (0, 1):
        w_ring(way, 1, 0).start()
    for part in PARTS:
        k_ring_in(part % 2, far, part).wait_recv()
        k_core(part % 2, far, part).start()

    def q_end(zz, carry):
        q_own(zz).wait()
        q_in(zz).wait_recv()
        return carry

    lax.fori_loop(0, units, q_end, 0)

    lane = lax.broadcasted_iota(jnp.int32, (chip, ROPE), 1)
    ones_lane = jnp.where(lane == 0, 1.0, 0.0).astype(jnp.bfloat16)
    scale = math.log2(math.e) / math.sqrt(NOPE + ROPE)

    def values(zz, turn):
        for j in range(heads):
            made[turn, :, j * VH : (j + 1) * VH] = jnp.dot(
                mixed[j * chip : (j + 1) * chip, :],
                w[zz, 1, :, j * VH : (j + 1) * VH],
                preferred_element_type=jnp.float32,
            ).astype(jnp.bfloat16)

    def unit(zz):
        block = q[:, pl.ds(pl.multiple_of(zz * q_wide, LANES), q_wide)]
        for j in range(heads):
            at = j * (NOPE + ROPE)
            row = j * chip
            lat = lax.dot_general(
                block[:, at : at + NOPE],
                w[zz, 0, :, j * NOPE : (j + 1) * NOPE],
                NT,
                preferred_element_type=jnp.float32,
            )
            qs[row : row + chip, :LATENT] = (lat * scale).astype(jnp.bfloat16)
            rot = block[:, at + NOPE : at + NOPE + ROPE].astype(jnp.float32)
            swapped = jnp.concatenate([rot[:, ROPE // 2 :], rot[:, : ROPE // 2]], 1)
            turned = (rot * turn_ref[:, :ROPE] + swapped * turn_ref[:, ROPE:]) * scale
            qs[row : row + chip, LATENT:] = jnp.concatenate(
                [turned.astype(jnp.bfloat16), ones_lane], 1
            )

        down_by = lax.broadcasted_iota(jnp.int32, (chip, LANES), 0) - lax.broadcasted_iota(
            jnp.int32, (chip, LANES), 1
        )
        down_by = jnp.concatenate([down_by] * heads, 0)
        best = None
        for first in range(0, keys_all, BLOCK):
            s = lax.dot_general(
                qs[...], keys[first : first + BLOCK, :], NT, preferred_element_type=jnp.float32
            )
            for n in range(0, BLOCK, LANES):
                tile = s[:, n : n + LANES]
                owner = (first + n - cached_all) // chip
                if owner >= 0:
                    tile = jnp.where(down_by >= (owner - z) * chip, tile, DEAD)
                scores[:, first + n : first + n + LANES] = tile
                best = tile if best is None else jnp.maximum(best, tile)
        best = jnp.broadcast_to(jnp.max(best, axis=1, keepdims=True), best.shape)
        total = None
        parts = []
        for first in range(0, keys_all, LANES):
            p = jnp.exp2(scores[:, first : first + LANES] - best)
            total = p if total is None else total + p
            parts.append(p.astype(jnp.bfloat16))
        acc = jnp.dot(
            jnp.concatenate(parts, 1), keys[:, :LATENT], preferred_element_type=jnp.float32
        )
        norm = 1.0 / jnp.sum(total, axis=1, keepdims=True)
        mixed[...] = (acc * norm).astype(jnp.bfloat16)

    def w_in(d, m):
        for way in (0, 1):

            @pl.when(jnp.logical_or(d < far, m == way))
            def _():
                w_ring_in(way, d, m).wait_recv()

                @pl.when(jnp.logical_or(d < far - 1, jnp.logical_and(d < far, m == way)))
                def _():
                    w_ring(way, d, m).start()

                w_side(way, d, m).start()

    def chip_of(u):
        return far_slot(1 - lax.rem(u, 2), (u + 1) // 2)

    def o_into(u, core):
        slot = chip_of(u) * 2 + core
        return out_hbm.at[:, pl.ds(pl.multiple_of(slot * o_wide, LANES), o_wide)]

    def o_own(u):
        return pltpu.make_async_copy(
            made.at[u, pl.ds(c * tok, tok)], o_into(u, c), ol_sem.at[u]
        )

    def o_out(u):
        return copy(made.at[u, pl.ds((1 - c) * tok, tok)], o_into(u, c), o_s.at[u], o_r.at[u], mate)

    def o_in(u):
        return copy(made.at[u, pl.ds(c * tok, tok)], o_into(u, 1 - c), o_s.at[u], o_r.at[u], mate)

    for part in PARTS:
        k_core_in(0, 0, part).wait_recv()

    def k_rest(d, carry):
        for part in PARTS:
            for way in (0, 1):
                k_core_in(way, d, part).wait_recv()
        return carry

    lax.fori_loop(1, far, k_rest, 0)
    for part in PARTS:
        k_core_in(part % 2, far, part).wait_recv()

    def step(u, carry):
        e = (u + 1) // 2
        odd = lax.rem(u, 2) == 1

        @pl.when(u == 1)
        def _():
            w_in(1, 1)

        for m in (0, 1):

            @pl.when(jnp.logical_and(odd == (m == 0), jnp.logical_and(u > 0, u < units - 1)))
            def _():
                w_in(e + 1, m)

        @pl.when(u > 0)
        def _():
            w_side_in(1 - lax.rem(u, 2), e, 0).wait_recv()

        @pl.when(u > 1)
        def _():
            o_own(u - 2).start()
            o_out(u - 2).start()
            values_in(u - 1)

        before = u - 1 + (units - u) // units
        values(chip_of(before), before)
        unit(chip_of(u))
        return carry

    def values_in(u):
        way = 1 - lax.rem(u, 2) + (u + 1) // units
        w_side_in(way, (u + 1) // 2, 1).wait_recv()

    mixed[...] = jnp.zeros_like(mixed)
    lax.fori_loop(0, units, step, 0)
    o_own(units - 2).start()
    o_out(units - 2).start()
    values_in(units - 1)
    values(chip_of(units - 1), units - 1)

    for part in PARTS:
        k_core(0, 0, part).wait_send()
        for way in (0, 1):
            k_ring(way, 0, part).wait_send()
    for m in (0, 1):
        for way in (0, 1):
            w_ring(way, 0, m).wait_send()
    o_own(units - 1).start()
    o_out(units - 1).start()

    def drain(d, carry):
        for way in (0, 1):
            for part in PARTS:

                @pl.when(jnp.logical_or(d < far - 1, part % 2 == way))
                def _():
                    k_ring(way, d, part).wait_send()

                k_core(way, d, part).wait_send()
            for m in (0, 1):

                @pl.when(jnp.logical_or(d < far - 1, m == way))
                def _():
                    w_ring(way, d, m).wait_send()

                w_side(way, d, m).wait_send()
        return carry

    lax.fori_loop(1, far, drain, 0)
    for part in PARTS:
        k_core(part % 2, far, part).wait_send()
    for m in (0, 1):
        w_side(m, far, m).wait_send()

    def finish(u, carry):
        q_out(u).wait_send()
        o_own(u).wait()
        o_out(u).wait_send()
        o_in(u).wait_recv()
        return carry

    lax.fori_loop(0, units, finish, 0)


def local(queries, kv_new, kv_cache, kv_gain, w_key, w_value, prefix_len):
    ring = lax.axis_size("z")
    tok = queries.shape[0]
    cache = kv_cache.shape[0]
    heads = w_key.shape[1] // NOPE
    slots = 2 * ring
    keys_all = slots * (cache + tok)
    rows_all = 2 * heads * tok
    hbm = pl.BlockSpec(memory_space=pl.ANY)
    vmem = pl.BlockSpec(memory_space=pltpu.VMEM)
    each = pltpu.SemaphoreType.DMA((ring,))
    sems = pltpu.SemaphoreType.DMA((2, ring // 2 + 1, 2))
    return pl.pallas_call(
        functools.partial(kernel, (ring, tok, cache, heads)),
        out_shape=jax.ShapeDtypeStruct((tok, slots * heads * VH), jnp.bfloat16),
        in_specs=[
            pl.BlockSpec(memory_space=pltpu.SMEM),
            hbm,
            vmem,
            vmem,
            vmem,
            hbm,
            hbm,
        ],
        out_specs=hbm,
        scratch_shapes=[
            pltpu.VMEM((ring, 2, LATENT, heads * NOPE), jnp.bfloat16),
            pltpu.VMEM((keys_all, WIDE), jnp.bfloat16),
            pltpu.VMEM((2 * tok, ring * heads * (NOPE + ROPE)), jnp.bfloat16),
            pltpu.VMEM((2 * tok, LANES), jnp.float32),
            pltpu.VMEM((rows_all, WIDE), jnp.bfloat16),
            pltpu.VMEM((rows_all, keys_all), jnp.float32),
            pltpu.VMEM((rows_all, LATENT), jnp.bfloat16),
            pltpu.VMEM((ring, 2 * tok, heads * VH), jnp.bfloat16),
            pltpu.SemaphoreType.DMA((2,)),
        ]
        + [each] * 6
        + [pltpu.SemaphoreType.DMA((2, ring // 2 + 1, len(PARTS)))] * 4
        + [sems] * 4,
        compiler_params=pltpu.CompilerParams(
            collective_id=0, has_side_effects=True, vmem_limit_bytes=66 * 1000 * 1000
        ),
        name="attend",
    )(prefix_len, queries, kv_new, kv_cache, kv_gain[None, :], w_key, w_value)


def solution(mesh):
    side = math.isqrt(mesh.shape["groups"])
    ring = mesh.shape["seq"] // 2
    torus = Mesh(mesh.devices.reshape(side // 2, 2, side // 2, 2, ring, 2), AXES)
    tokens = P((*GROUPS, *SEQ), None)
    placed = (tokens, tokens, tokens, P(), P(None, SEQ), P(None, SEQ), P(GROUPS))
    return jax.shard_map(local, mesh=torus, in_specs=placed, out_specs=tokens, check_vma=False)
```
